32 devices in a mesh: seq: 16 (over z, y, core), head: 2 (over x).
Axes of the slice: x: 2, y: 2, z: 4, core: 2. Of those that a mesh axis runs over, the one named last changes fastest.
Arguments:
- queries: bfloat16 [4096, 4096], P('seq', 'head'), may hold values from -8 to 8
- keys: bfloat16 [4096, 2048], P('seq', 'head'), may hold values from -8 to 8
- values: bfloat16 [4096, 2048], P('seq', 'head'), may hold values from -6 to 6
- segment_ids: int32 [4096], P(('seq', 'head')), may hold values from 0 to 7, never falling along the last dimension, each value on 1 to 2048 neighbouring positions
Outputs:
- attended: bfloat16 [4096, 4096], P('seq', 'head')
The draws below stay inside these ranges and needn't reach their ends.
Inputs may be any that keep to these rules, and one draw needn't show every extreme that they name: `segment_ids`: document numbers never fall along the tokens; each document has 1 to 2048 tokens, one exactly 2048.
All inputs are finite; a program needn't handle non-finite values.
Results may differ from the reference program's by a relative error of at most 0.0037.
Values may be sent and summed in bfloat16 or wider, within the bound.
No kernel may reach another device: no remote copies, remote signals or barrier semaphores. Data moves between devices by JAX's collectives and lax.ppermute only.
A program may use at most 64 MiB of HBM per device.

```python
import math
import jax
import jax.numpy as jnp
import numpy as np
from jax import lax

HQ = 32
KEY_VALUE_HEADS = 16
HEAD_WIDTH = 128
WINDOW = 1024
TOK_DEV = 256
MOST = 2048
PACKED_TOKENS = 4096
COUNT = 8
N_SEQ = 16


def draw_queries(key, part):
    final_output = jnp.clip(jax.random.normal(jax.random.fold_in(key, 1), (PACKED_TOKENS, HQ * HEAD_WIDTH)), -8.0, 8.0)
    return final_output.astype(jnp.bfloat16)


def draw_keys(key, part):
    final_output = jnp.clip(jax.random.normal(jax.random.fold_in(key, 2), (PACKED_TOKENS, KEY_VALUE_HEADS * HEAD_WIDTH)), -8.0, 8.0)
    return final_output.astype(jnp.bfloat16)


def block_scale(rng, dims, shards, smallest, largest):
    gain = 1.0
    for dim, shards_of in shards:
        draws = jax.random.uniform(jax.random.fold_in(jax.random.fold_in(rng, 6), dim), (shards_of,), jnp.float32, smallest / len(shards), largest / len(shards))
        gain = gain * jnp.repeat(jnp.exp(draws), dims[dim] // shards_of).reshape((-1,) + (1,) * (len(dims) - 1 - dim))
    return gain


def length_profile(count, total, reach, skew):
    loads = [(1 << 20) // math.isqrt(grade ** skew) + 1 for grade in range(2, count + 1)]
    rest, holding = total - reach - (count - 1), [1] * (count - 1)
    while rest > 0:
        candidates = [i for i in range(count - 1) if holding[i] < reach]
        whole, remaining = sum([loads[i] for i in candidates]), rest
        for i in candidates:
            addition = min(reach - holding[i], max(1, remaining * loads[i] // whole), rest)
            holding[i] = holding[i] + addition
            rest = rest - addition
    return np.array([reach] + holding)


def ragged(own_key, count, total, limit, lean):
    if count == 2:
        one = jax.random.randint(own_key, (), max(1, total - limit), min(limit, total - 1) + 1)
        return jnp.stack([one, total - one])
    sizes = jnp.asarray(length_profile(count, total, limit, lean), jnp.int32)
    twos = (count - 1) // 2
    donor, taker = sizes[1:1 + 2 * twos:2], sizes[2:2 + 2 * twos:2]
    margin = jnp.minimum(donor - 1, limit - taker)
    moved = jax.random.randint(jax.random.fold_in(own_key, 1), (twos,), 0, 1 << 20) % (margin + 1)
    sizes = sizes.at[1:1 + 2 * twos:2].set(donor - moved).at[2:2 + 2 * twos:2].set(taker + moved)
    return sizes[jax.random.permutation(jax.random.fold_in(own_key, 2), count)]


def scatter_about(rng, dims, spread, limit, split=(), kind=jnp.bfloat16):
    result = spread * jax.random.normal(rng, dims, jnp.float32)
    if split:
        result = result * block_scale(rng, dims, split, -0.22, 0.18)
    return jnp.clip(result, -limit, limit).astype(kind)


def setup_inputs(seed: int = 0) -> dict:
    arg_keys = jax.random.split(jax.random.key(seed), 5)
    queries = draw_queries(jax.random.fold_in(arg_keys[4], 71), 0)
    keys = draw_keys(jax.random.fold_in(arg_keys[4], 71), 0)
    values = scatter_about(arg_keys[2], (PACKED_TOKENS, KEY_VALUE_HEADS * HEAD_WIDTH), 1.0, 6.0, ((0, 16), (1, 2)))
    segment_ids = jnp.searchsorted(jnp.cumsum(ragged(arg_keys[3], COUNT, PACKED_TOKENS, MOST, 2)), jnp.arange(PACKED_TOKENS), side="right").astype(jnp.int32)
    return {"queries": queries, "keys": keys, "values": values, "segment_ids": segment_ids}


score_scale = 168.0 ** -0.5


def attend(queries, keys, values, query_ids, key_ids, query_pos, key_pos):
    tok_rows = queries.shape[0]
    span = keys.shape[0]
    kv_heads = keys.shape[1] // HEAD_WIDTH
    group = queries.shape[1] // keys.shape[1]
    visible = (key_ids[None, :] == query_ids[:, None]) & (key_pos[None, :] <= query_pos[:, None]) & (query_pos[:, None] - key_pos[None, :] < WINDOW)
    grouped_q = queries.reshape(tok_rows, kv_heads, group, HEAD_WIDTH).transpose(1, 0, 2, 3)
    grouped_k = keys.reshape(span, kv_heads, HEAD_WIDTH).transpose(1, 0, 2)
    grouped_v = values.reshape(span, kv_heads, HEAD_WIDTH).transpose(1, 0, 2)

    def one_head(operands):
        head_q, head_k, head_v = operands
        scores = jnp.einsum('tgd,sd->gts', head_q.astype(jnp.float32), head_k.astype(jnp.float32)) * score_scale
        scores = jnp.where(visible[None], scores, -1e30)
        top = jnp.max(scores, axis=2, keepdims=True)
        weights = jnp.exp(scores - top)
        total = jnp.sum(weights, axis=2)
        rounded = weights.astype(jnp.bfloat16)
        mixed = jnp.einsum('gts,sd->tgd', rounded.astype(jnp.float32), head_v.astype(jnp.float32))
        return (mixed / total.T[:, :, None]).astype(jnp.bfloat16)

    final_output = lax.map(one_head, (grouped_q, grouped_k, grouped_v))
    return final_output.transpose(1, 0, 2, 3).reshape(tok_rows, -1)


def reference(queries, keys, values, segment_ids):
    padded_k = jnp.concatenate([jnp.zeros((WINDOW, keys.shape[1]), keys.dtype), keys])
    padded_v = jnp.concatenate([jnp.zeros((WINDOW, values.shape[1]), values.dtype), values])
    padded_ids = jnp.concatenate([jnp.full((WINDOW,), -1, jnp.int32), segment_ids.astype(jnp.int32)])
    span = WINDOW + TOK_DEV
    query_pos = jnp.arange(TOK_DEV, dtype=jnp.int32)
    key_pos = jnp.arange(span, dtype=jnp.int32) - WINDOW

    def block(index):
        start = (index * TOK_DEV).astype(jnp.int32)
        block_q = lax.dynamic_slice_in_dim(queries, start, TOK_DEV, 0)
        block_ids = lax.dynamic_slice_in_dim(segment_ids.astype(jnp.int32), start, TOK_DEV, 0)
        block_k = lax.dynamic_slice_in_dim(padded_k, start, span, 0)
        block_v = lax.dynamic_slice_in_dim(padded_v, start, span, 0)
        key_ids = lax.dynamic_slice_in_dim(padded_ids, start, span, 0)
        return attend(block_q, block_k, block_v, block_ids, key_ids, query_pos, key_pos)

    final_output = lax.map(block, jnp.arange(N_SEQ, dtype=jnp.int32))
    return final_output.reshape(PACKED_TOKENS, -1)
```

```python
import functools
import math

import jax
import jax.numpy as jnp
from jax import lax
from jax.experimental import pallas as pl
from jax.experimental.pallas import tpu as pltpu
from jax.sharding import PartitionSpec as P

HEAD_WIDTH = 128
WINDOW = 1024
HIDDEN = -1e30
EXPONENT_SCALE = 168.0 ** (-0.5) * math.log2(math.e)


def weights_kernel(q_ref, k0, k1, k2, k3, k4, i0, i1, i2, i3, i4, p_ref, total_ref, bias):
    tok_rows = k0.shape[0]
    group = q_ref.shape[1] // HEAD_WIDTH

    @pl.when(pl.program_id(0) == 0)
    def _():
        own = jnp.broadcast_to(i0[...], (tok_rows, tok_rows)).T
        row = lax.broadcasted_iota(jnp.int32, (tok_rows, tok_rows), 0)
        col = lax.broadcasted_iota(jnp.int32, (tok_rows, tok_rows), 1)
        for b, ids in enumerate((i0, i1, i2, i3, i4)):
            seen = ids[...] == own
            if b == 0:
                seen = seen & (col <= row)
            if b == 1:
                seen = seen & (col > row)
            bias[b] = jnp.where(seen, 0.0, HIDDEN)

    q = jnp.concatenate([q_ref[:, g * HEAD_WIDTH:(g + 1) * HEAD_WIDTH] for g in range(group)], axis=0)
    scores = []
    for b, k in enumerate((k0, k1, k2, k3, k4)):
        s = lax.dot_general(q, k[...], (((1,), (1,)), ((), ())), preferred_element_type=jnp.float32)
        s = s.reshape(group, tok_rows, tok_rows) * EXPONENT_SCALE + bias[b][None]
        scores.append(s.reshape(group * tok_rows, tok_rows))
    top = functools.reduce(jnp.maximum, scores)
    top = jnp.max(top, axis=1, keepdims=True)
    sums = None
    for b, s in enumerate(scores):
        w = jnp.exp2(s - top)
        sums = w if sums is None else sums + w
        p_ref[0, :, b * tok_rows:(b + 1) * tok_rows] = w.astype(jnp.bfloat16)
    total = jnp.sum(sums, axis=1, keepdims=True)
    total_ref[0] = jnp.broadcast_to(total, (group * tok_rows, HEAD_WIDTH))


def weights(queries, blocks, ids):
    tok_rows = queries.shape[0]
    kv_heads = blocks[0].shape[1] // HEAD_WIDTH
    group = queries.shape[1] // blocks[0].shape[1]
    span = len(blocks) * tok_rows
    k_spec = pl.BlockSpec((tok_rows, HEAD_WIDTH), lambda h: (0, h))
    i_spec = pl.BlockSpec((1, tok_rows), lambda h: (0, 0))
    return pl.pallas_call(
        weights_kernel,
        grid=(kv_heads,),
        in_specs=[pl.BlockSpec((tok_rows, group * HEAD_WIDTH), lambda h: (0, h))] + [k_spec] * 5 + [i_spec] * 5,
        out_specs=[
            pl.BlockSpec((1, group * tok_rows, span), lambda h: (h, 0, 0)),
            pl.BlockSpec((1, group * tok_rows, HEAD_WIDTH), lambda h: (h, 0, 0)),
        ],
        out_shape=[
            jax.ShapeDtypeStruct((kv_heads, group * tok_rows, span), jnp.bfloat16),
            jax.ShapeDtypeStruct((kv_heads, group * tok_rows, HEAD_WIDTH), jnp.float32),
        ],
        scratch_shapes=[pltpu.VMEM((5, tok_rows, tok_rows), jnp.float32)],
        cost_estimate=pl.CostEstimate(
            flops=2 * queries.size * span, transcendentals=queries.size // HEAD_WIDTH * span, bytes_accessed=queries.size * 2),
        name="weights",
    )(queries, *blocks, *ids)


def first_kernel(p_ref, v0, v1, v2, acc_ref):
    tok_rows = v0.shape[0]
    acc = None
    for b, v in enumerate((v0, v1, v2)):
        d = jnp.dot(p_ref[0, :, b * tok_rows:(b + 1) * tok_rows], v[...], preferred_element_type=jnp.float32)
        acc = d if acc is None else acc + d
    acc_ref[0] = acc


def first(p, blocks):
    kv_heads, rows, span = p.shape
    tok_rows = blocks[0].shape[0]
    v_spec = pl.BlockSpec((tok_rows, HEAD_WIDTH), lambda h: (0, h))
    return pl.pallas_call(
        first_kernel,
        grid=(kv_heads,),
        in_specs=[pl.BlockSpec((1, rows, 3 * tok_rows), lambda h: (h, 0, 0))] + [v_spec] * 3,
        out_specs=pl.BlockSpec((1, rows, HEAD_WIDTH), lambda h: (h, 0, 0)),
        out_shape=jax.ShapeDtypeStruct((kv_heads, rows, HEAD_WIDTH), jnp.float32),
        cost_estimate=pl.CostEstimate(flops=2 * kv_heads * rows * 3 * tok_rows * HEAD_WIDTH, transcendentals=0, bytes_accessed=p.size),
        name="first",
    )(p, *blocks)


def last_kernel(p3, p4, v3, v4, acc_ref, total_ref, out_ref):
    tok_rows = v3.shape[0]
    group = out_ref.shape[1] // HEAD_WIDTH
    acc = acc_ref[0]
    acc = acc + jnp.dot(p3[0], v3[...], preferred_element_type=jnp.float32)
    acc = acc + jnp.dot(p4[0], v4[...], preferred_element_type=jnp.float32)
    out = (acc / total_ref[0]).astype(out_ref.dtype)
    for g in range(group):
        out_ref[:, g * HEAD_WIDTH:(g + 1) * HEAD_WIDTH] = out[g * tok_rows:(g + 1) * tok_rows]


def last(p, blocks, acc, total):
    kv_heads, rows, span = p.shape
    tok_rows = blocks[0].shape[0]
    group = rows // tok_rows
    v_spec = pl.BlockSpec((tok_rows, HEAD_WIDTH), lambda h: (0, h))
    a_spec = pl.BlockSpec((1, rows, HEAD_WIDTH), lambda h: (h, 0, 0))
    return pl.pallas_call(
        last_kernel,
        grid=(kv_heads,),
        in_specs=[
            pl.BlockSpec((1, rows, tok_rows), lambda h: (h, 0, 3)),
            pl.BlockSpec((1, rows, tok_rows), lambda h: (h, 0, 4)),
            v_spec, v_spec, a_spec, a_spec],
        out_specs=pl.BlockSpec((tok_rows, group * HEAD_WIDTH), lambda h: (0, h)),
        out_shape=jax.ShapeDtypeStruct((tok_rows, kv_heads * group * HEAD_WIDTH), jnp.bfloat16),
        cost_estimate=pl.CostEstimate(flops=2 * kv_heads * rows * 2 * tok_rows * HEAD_WIDTH, transcendentals=0, bytes_accessed=p.size),
        name="last",
    )(p, p, *blocks, acc, total)


def body(queries, keys, values, segment_ids):
    tok_rows = keys.shape[0]
    reach = WINDOW // tok_rows
    count = lax.axis_size("seq")
    assert reach == 4 and reach * tok_rows == WINDOW and count % reach == 0
    place = lax.axis_index("seq") % reach
    ahead = [(i, i + reach) for i in range(count - reach)]
    across = [(i, i ^ 2) for i in range(count)]
    beside = [(i, i ^ 1) for i in range(count)]

    def send(x, pairs):
        return lax.ppermute(x, "seq", pairs)

    key_far = send(keys, ahead)
    value_far = send(values, ahead)
    own_ids = lax.all_gather(segment_ids, "head", axis=0, tiled=True) + 1
    id_far = send(own_ids, ahead)

    def spread(own, far):
        two = send(jnp.where(place >= 2, far, own), across)
        one = send(jnp.where(place % 2 == 1, far, own), beside)
        three = send(two, beside)
        return own, far, one, two, three

    ids = [x[None] for x in spread(own_ids, id_far)]
    ks = spread(keys, key_far)
    p, total = weights(queries, ks, ids)
    vs = spread(values, value_far)
    acc = first(p, vs[:3])
    return last(p, vs[3:], acc, total)


def solution(mesh):
    in_specs = (P("seq", "head"), P("seq", "head"), P("seq", "head"), P(("seq", "head")))
    out_specs = P("seq", "head")
    return jax.shard_map(body, mesh=mesh, in_specs=in_specs, out_specs=out_specs, check_vma=False)
```

```python
import functools
import math

import jax
import jax.numpy as jnp
from jax import lax
from jax.experimental import pallas as pl
from jax.experimental.pallas import tpu as pltpu
from jax.sharding import PartitionSpec as P


HEAD_WIDTH = 128
WINDOW = 1024
HIDDEN = -1e30
EXPONENT_SCALE = 168.0 ** (-0.5) * math.log2(math.e)
MIB = 1 << 20


def lanes(h, width=HEAD_WIDTH):
    return pl.ds(pl.multiple_of(h * width, width), width)


def weights_kernel(q_ref, k0, k1, k2, k3, k4, i0, i1, i2, i3, i4, p_ref, total_ref, bias):
    tok_rows = k0.shape[0]
    kv_heads = k0.shape[1] // HEAD_WIDTH
    group = q_ref.shape[1] // k0.shape[1]
    own = jnp.broadcast_to(i0[...], (tok_rows, tok_rows)).T
    row = lax.broadcasted_iota(jnp.int32, (tok_rows, tok_rows), 0)
    col = lax.broadcasted_iota(jnp.int32, (tok_rows, tok_rows), 1)
    for b, ids in enumerate((i0, i1, i2, i3, i4)):
        seen = ids[...] == own
        if b == 0:
            seen = seen & (col <= row)
        if b == 1:
            seen = seen & (col > row)
        bias[b] = jnp.where(seen, 0.0, HIDDEN)

    @pl.loop(0, kv_heads)
    def _(h):
        q = q_ref[:, lanes(h, group * HEAD_WIDTH)]
        q = jnp.concatenate([q[:, g * HEAD_WIDTH:(g + 1) * HEAD_WIDTH] for g in range(group)], axis=0)
        scores = []
        for b, k in enumerate((k0, k1, k2, k3, k4)):
            s = lax.dot_general(q, k[:, lanes(h)], (((1,), (1,)), ((), ())), preferred_element_type=jnp.float32)
            s = s.reshape(group, tok_rows, tok_rows) * EXPONENT_SCALE + bias[b][None]
            scores.append(s.reshape(group * tok_rows, tok_rows))
        top = functools.reduce(jnp.maximum, scores)
        top = jnp.max(top, axis=1, keepdims=True)
        sums = None
        for b, s in enumerate(scores):
            w = jnp.exp2(s - top)
            sums = w if sums is None else sums + w
            p_ref[h, :, b * tok_rows:(b + 1) * tok_rows] = w.astype(jnp.bfloat16)
        total = jnp.sum(sums, axis=1, keepdims=True)
        total_ref[h] = jnp.broadcast_to(total, (group * tok_rows, HEAD_WIDTH))


def here(x):
    return pltpu.with_memory_space_constraint(x, pltpu.VMEM)


VMEM_SPEC = pl.BlockSpec(memory_space=pltpu.VMEM)


def weights(queries, blocks, ids):
    tok_rows = queries.shape[0]
    kv_heads = blocks[0].shape[1] // HEAD_WIDTH
    group = queries.shape[1] // blocks[0].shape[1]
    span = len(blocks) * tok_rows
    operands = [here(x) for x in (queries, *blocks, *ids)]
    return pl.pallas_call(
        weights_kernel,
        in_specs=[VMEM_SPEC] * len(operands),
        out_specs=[VMEM_SPEC] * 2,
        out_shape=[
            pltpu.VMEM((kv_heads, group * tok_rows, span), jnp.bfloat16),
            pltpu.VMEM((kv_heads, group * tok_rows, HEAD_WIDTH), jnp.float32),
        ],
        scratch_shapes=[pltpu.VMEM((5, tok_rows, tok_rows), jnp.float32)],
        compiler_params=pltpu.CompilerParams(vmem_limit_bytes=12 * MIB),
        cost_estimate=pl.CostEstimate(
            flops=2 * queries.size * span, transcendentals=queries.size // HEAD_WIDTH * span, bytes_accessed=queries.size * 2),
        name="weights",
    )(*operands)


def first_kernel(p_ref, v0, v1, v2, acc_ref):
    tok_rows = v0.shape[0]

    @pl.loop(0, p_ref.shape[0])
    def _(h):
        acc = None
        for b, v in enumerate((v0, v1, v2)):
            d = jnp.dot(p_ref[h, :, b * tok_rows:(b + 1) * tok_rows], v[:, lanes(h)], preferred_element_type=jnp.float32)
            acc = d if acc is None else acc + d
        acc_ref[h] = acc


def first(p, blocks):
    kv_heads, rows, _ = p.shape
    tok_rows = blocks[0].shape[0]
    operands = [here(x) for x in (p, *blocks)]
    return pl.pallas_call(
        first_kernel,
        in_specs=[VMEM_SPEC] * len(operands),
        out_specs=VMEM_SPEC,
        out_shape=pltpu.VMEM((kv_heads, rows, HEAD_WIDTH), jnp.float32),
        compiler_params=pltpu.CompilerParams(vmem_limit_bytes=4 * MIB),
        cost_estimate=pl.CostEstimate(flops=2 * kv_heads * rows * 3 * tok_rows * HEAD_WIDTH, transcendentals=0, bytes_accessed=p.size),
        name="first",
    )(*operands)


def last_kernel(p_ref, v3, v4, acc_ref, total_ref, out_ref, done, sems):
    tok_rows = v3.shape[0]
    kv_heads = p_ref.shape[0]
    group = out_ref.shape[1] // HEAD_WIDTH // kv_heads

    def copy(h):
        return pltpu.make_async_copy(done.at[h], out_ref.at[:, lanes(h, group * HEAD_WIDTH)], sems.at[h])

    @pl.loop(0, kv_heads)
    def _(h):
        acc = acc_ref[h]
        for b, v in ((3, v3), (4, v4)):
            acc = acc + jnp.dot(p_ref[h, :, b * tok_rows:(b + 1) * tok_rows], v[:, lanes(h)], preferred_element_type=jnp.float32)
        out = (acc / total_ref[h]).astype(out_ref.dtype)
        for g in range(group):
            done[h, :, g * HEAD_WIDTH:(g + 1) * HEAD_WIDTH] = out[g * tok_rows:(g + 1) * tok_rows]
        copy(h).start()

    @pl.loop(0, kv_heads)
    def _(h):
        copy(h).wait()


def last(p, blocks, acc, total):
    kv_heads, rows, _ = p.shape
    tok_rows = blocks[0].shape[0]
    group = rows // tok_rows
    operands = [here(x) for x in (p, *blocks, acc, total)]
    return pl.pallas_call(
        last_kernel,
        in_specs=[VMEM_SPEC] * len(operands),
        out_specs=pl.BlockSpec(memory_space=pl.ANY),
        out_shape=jax.ShapeDtypeStruct((tok_rows, kv_heads * group * HEAD_WIDTH), jnp.bfloat16),
        scratch_shapes=[
            pltpu.VMEM((kv_heads, tok_rows, group * HEAD_WIDTH), jnp.bfloat16),
            pltpu.SemaphoreType.DMA((kv_heads,)),
        ],
        compiler_params=pltpu.CompilerParams(vmem_limit_bytes=4 * MIB),
        cost_estimate=pl.CostEstimate(flops=2 * kv_heads * rows * 2 * tok_rows * HEAD_WIDTH, transcendentals=0, bytes_accessed=p.size),
        name="last",
    )(*operands)


def body(queries, keys, values, segment_ids):
    tok_rows = keys.shape[0]
    reach = WINDOW // tok_rows
    count = lax.axis_size("seq")
    assert reach == 4 and reach * tok_rows == WINDOW and count % reach == 0
    place = lax.axis_index("seq") % reach
    ahead = [(i, i + reach) for i in range(count - reach)]
    across = [(i, i ^ 2) for i in range(count)]
    beside = [(i, i ^ 1) for i in range(count)]

    def send(x, pairs, axis="seq"):
        return lax.ppermute(x, axis, pairs)

    heads = lax.axis_size("head")
    half = segment_ids + 1
    key_far = send(keys, ahead)
    value_far = send(values, ahead)
    if heads == 2:
        other = send(half, [(0, 1), (1, 0)], "head")
        low = lax.axis_index("head") == 0
        own_ids = jnp.concatenate([jnp.where(low, half, other), jnp.where(low, other, half)])
    else:
        own_ids = lax.all_gather(half, "head", axis=0, tiled=True)
    id_far = send(own_ids, ahead)

    def spread(own, far):
        two = send(jnp.where(place >= 2, far, own), across)
        one = send(jnp.where(place % 2 == 1, far, own), beside)
        three = send(two, beside)
        return own, far, one, two, three

    ks = spread(keys, key_far)
    ids = [x[None] for x in spread(own_ids, id_far)]
    vs = spread(values, value_far)
    p, total = weights(queries, ks, ids)
    acc = first(p, vs[:3])
    return last(p, vs[3:], acc, total)


def solution(mesh):
    in_specs = (P("seq", "head"), P("seq", "head"), P("seq", "head"), P(("seq", "head")))
    out_specs = P("seq", "head")
    return jax.shard_map(body, mesh=mesh, in_specs=in_specs, out_specs=out_specs, check_vma=False)
```
